32 devices in a mesh: gx: 4 (over z), gy: 8 (over y, x, core).
Axes of the slice: x: 2, y: 2, z: 4, core: 2. Of those that a mesh axis runs over, the one named last changes fastest.
Arguments:
- coarse_map: float32 [4, 8, 2, 128, 128], P('gx', 'gy'), may hold values from -0.675 to 0.675, as said below
- fine_maps: float32 [4, 8, 4, 2, 64, 64], P('gx', 'gy'), may hold values from -0.706066 to 0.706066, as said below
- pml_flag: int32 [4, 8], P('gx', 'gy'), may hold values 0 or 1
Outputs:
- top_map: float32 [2, 512, 1024], P(None, 'gx', 'gy')
The draws below stay inside these ranges and needn't reach their ends.
Inputs may be any that keep to these rules, and one draw needn't show every extreme that they name: `coarse_map`: every interface system met in the merges is well conditioned. `fine_maps`: every interface system met in the merges is well conditioned.
All inputs are finite; a program needn't handle non-finite values. No bound on the sum of `pml_flag` on one device may be relied on, other than what follows from the above.
Results may differ from the reference program's by a relative error of at most 0.0003.
Values sent between devices are 32-bit elements; how exact they have to be, the bound alone decides.
A program may use at most 64 MiB of HBM per device.

```python
import math
from functools import partial
import jax
import jax.numpy as jnp
import numpy as np
from jax import lax

E = 32
N_GX = 4
N_GY = 8


def noisy_maps(key, shape, perimeter):
    noise_key = jax.random.fold_in(key, 1)
    phase_key = jax.random.fold_in(key, 2)
    noise = jnp.clip(jax.random.normal(noise_key, shape, jnp.float32), -4.0, 4.0)
    noise = noise * (0.3 / math.sqrt(2.0 * perimeter))
    leading = shape[:-3]
    phases = jax.random.uniform(phase_key, leading + (perimeter,), jnp.float32, -math.pi, math.pi)
    identity = jnp.eye(perimeter, dtype=jnp.float32)
    centre_real = (-0.6 * jnp.cos(phases))[..., :, None] * identity
    centre_imag = (-0.6 * jnp.sin(phases))[..., :, None] * identity
    centre = jnp.stack([centre_real, centre_imag], axis=-3)
    return noise + centre


def draw_coarse_map(key, part):
    return noisy_maps(jax.random.fold_in(key, 11), (N_GX, N_GY, 2, 4 * E, 4 * E), 4 * E)


def draw_fine_maps(key, part):
    return noisy_maps(jax.random.fold_in(key, 23), (N_GX, N_GY, 4, 2, 2 * E, 2 * E), 2 * E)


def with_ends(entries, own_key, low, top_value):
    place = [jax.random.randint(jax.random.fold_in(own_key, axis), (), 0, length) for axis, length in enumerate(entries.shape)]
    widest = entries.shape.index(max(entries.shape))
    beside = place[:widest] + [(place[widest] + 1) % entries.shape[widest]] + place[widest + 1:]
    return entries.at[tuple(place)].set(low).at[tuple(beside)].set(top_value)


def setup_inputs(seed: int = 0) -> dict:
    key_list = jax.random.split(jax.random.key(seed), 4)
    return {
        "coarse_map": draw_coarse_map(jax.random.fold_in(key_list[3], 71), 0),
        "fine_maps": draw_fine_maps(jax.random.fold_in(key_list[3], 71), 0),
        "pml_flag": with_ends((jax.random.randint(key_list[2], (N_GX, N_GY), 0, 4) < 1).astype(jnp.int32), jax.random.fold_in(key_list[2], 1), 0, 1),
    }


def box_labels(anchor_x, anchor_y, across, upward):
    south = [(0, anchor_y, anchor_x + offset) for offset in range(across)]
    east = [(1, anchor_x + across, anchor_y + offset) for offset in range(upward)]
    north = [(0, anchor_y + upward, anchor_x + offset) for offset in range(across)]
    west = [(1, anchor_x, anchor_y + offset) for offset in range(upward)]
    return south + east + north + west

def pair_tables(former, latter):
    where_latter = {marker: position for position, marker in enumerate(latter)}
    shared = set(former) & set(latter)
    outer_a = [position for position, marker in enumerate(former) if marker not in shared]
    inner_a = [position for position, marker in enumerate(former) if marker in shared]
    inner_b = [where_latter[former[position]] for position in inner_a]
    outer_b = [position for position, marker in enumerate(latter) if marker not in shared]
    joined = [former[position] for position in outer_a] + [latter[position] for position in outer_b]
    tables = (np.array(outer_a), np.array(inner_a), np.array(outer_b), np.array(inner_b))
    return (tables, joined)

def level_tables(points):
    offsets = [(0, points), (points, 0), (0, 2 * points), (2 * points, 0)]

    def labels_at(section, anchor_x, anchor_y):
        if section == 0:
            return box_labels(anchor_x, anchor_y, points, points)
        shift_x, shift_y = offsets[section - 1]
        former = labels_at(section - 1, anchor_x, anchor_y)
        latter = labels_at(section - 1, anchor_x + shift_x, anchor_y + shift_y)
        return pair_tables(former, latter)[1]
    sections = []
    for section in range(1, 5):
        shift_x, shift_y = offsets[section - 1]
        sections.append(pair_tables(labels_at(section - 1, 0, 0), labels_at(section - 1, shift_x, shift_y))[0])
    return sections

def fine_tables(points):
    halved = points // 2
    left_tab, left_join = pair_tables(box_labels(0, 0, halved, halved), box_labels(0, halved, halved, halved))
    right_tab, right_join = pair_tables(box_labels(halved, 0, halved, halved), box_labels(halved, halved, halved, halved))
    whole_tab, whole_join = pair_tables(left_join, right_join)
    where_whole = {marker: position for position, marker in enumerate(whole_join)}
    order = np.array([where_whole[marker] for marker in box_labels(0, 0, points, points)])
    return (left_tab, right_tab, whole_tab, order)

def real_dot(left_part, right_part):
    return jnp.dot(left_part.astype(jnp.float32), right_part.astype(jnp.float32), precision=lax.Precision.HIGHEST, preferred_element_type=jnp.float32)

def complex_dot(left_part, right_part):
    real_part = real_dot(left_part[0], right_part[0]) - real_dot(left_part[1], right_part[1])
    imaginary = real_dot(left_part[0], right_part[1]) + real_dot(left_part[1], right_part[0])
    return jnp.stack([real_part, imaginary])

def complex_solve(system, right_side):
    upper = jnp.concatenate([system[0], -system[1]], axis=1)
    lower = jnp.concatenate([system[1], system[0]], axis=1)
    stacked = jnp.concatenate([upper, lower], axis=0)
    loads_real = jnp.concatenate([right_side[0], right_side[1]], axis=0)
    normal_matrix = real_dot(stacked.T, stacked)
    factor = jnp.linalg.cholesky(normal_matrix)
    solved = jax.scipy.linalg.cho_solve((factor, True), real_dot(stacked.T, loads_real))
    half_rows = right_side.shape[1]
    return jnp.stack([solved[:half_rows], solved[half_rows:]])

def zero_block(size_rows, size_cols):
    return jnp.zeros((2, size_rows, size_cols), jnp.float32)

def interface_solve(inner_former, inward_former, inner_latter, inward_latter):
    size_inner = inner_former.shape[1]
    product = complex_dot(inner_latter, inner_former)
    system = jnp.stack([jnp.eye(size_inner, dtype=jnp.float32) - product[0], -product[1]])
    right_side = jnp.concatenate([complex_dot(inner_latter, inward_former), -inward_latter], axis=2)
    return complex_solve(system, right_side)

def merge_pair(former, latter, tables):
    outer_a, inner_a, outer_b, inner_b = tables
    outer_former = former[:, outer_a][:, :, outer_a]
    coupling_former = former[:, outer_a][:, :, inner_a]
    inward_former = former[:, inner_a][:, :, outer_a]
    inner_former = former[:, inner_a][:, :, inner_a]
    outer_latter = latter[:, outer_b][:, :, outer_b]
    coupling_latter = latter[:, outer_b][:, :, inner_b]
    inward_latter = latter[:, inner_b][:, :, outer_b]
    inner_latter = latter[:, inner_b][:, :, inner_b]
    size_former = len(outer_a)
    size_latter = len(outer_b)
    size_inner = len(inner_a)
    solved = interface_solve(inner_former, inward_former, inner_latter, inward_latter)
    upper_rows = jnp.concatenate([outer_former, zero_block(size_former, size_latter)], axis=2) + complex_dot(coupling_former, solved)
    traces = jnp.concatenate([inward_former, zero_block(size_inner, size_latter)], axis=2) + complex_dot(inner_former, solved)
    lower_rows = jnp.concatenate([zero_block(size_latter, size_former), outer_latter], axis=2) - complex_dot(coupling_latter, traces)
    return jnp.concatenate([upper_rows, lower_rows], axis=1)

def fine_merge(pieces, fine_set):
    left_tab, right_tab, whole_tab, order = fine_set
    left_map = merge_pair(pieces[0], pieces[1], left_tab)
    right_map = merge_pair(pieces[2], pieces[3], right_tab)
    whole = merge_pair(left_map, right_map, whole_tab)
    return whole[:, order][:, :, order]

def merge_all(former, latter, tables):
    leading = former.shape[:2]
    merged = jax.vmap(partial(merge_pair, tables=tables))(former.reshape((-1,) + former.shape[2:]), latter.reshape((-1,) + latter.shape[2:]))
    return merged.reshape(leading + merged.shape[1:])

def reference(coarse_map, fine_maps, pml_flag):
    points = coarse_map.shape[-1] // 4
    fine_set = fine_tables(points)
    sections = level_tables(points)
    flat_coarse = coarse_map.reshape((N_GX * N_GY,) + coarse_map.shape[2:])
    flat_fine = fine_maps.reshape((N_GX * N_GY,) + fine_maps.shape[2:])
    refined = lax.map(partial(fine_merge, fine_set=fine_set), flat_fine)
    flag_rows = pml_flag.reshape(-1)
    box_maps = jnp.where(flag_rows[:, None, None, None] > 0, refined, flat_coarse)
    box_maps = box_maps.reshape((N_GX, N_GY) + coarse_map.shape[2:])
    section_one = merge_all(box_maps[:, 0::2], box_maps[:, 1::2], sections[0])
    section_two = merge_all(section_one[0::2], section_one[1::2], sections[1])
    section_three = merge_all(section_two[:, 0::2], section_two[:, 1::2], sections[2])
    section_four = merge_all(section_three[0::2], section_three[1::2], sections[3])
    return section_four.transpose(2, 0, 3, 1, 4).reshape(2, N_GX * 4 * points, N_GY * 4 * points)
```

```python
import functools
import jax
import jax.numpy as jnp
import numpy as np
from jax import lax
from jax.experimental import pallas as pl
from jax.experimental.pallas import tpu as pltpu
from jax.sharding import PartitionSpec as P

def partner(block, axis, stride):
    count = lax.axis_size(axis)
    route = []
    for low in range(count):
        high = low | 1 << stride
        if high != low and high < count:
            route += [(low, high), (high, low)]
    return lax.ppermute(block, axis, route)


def box_labels(anchor_x, anchor_y, across, upward):
    south = [(0, anchor_y, anchor_x + offset) for offset in range(across)]
    east = [(1, anchor_x + across, anchor_y + offset) for offset in range(upward)]
    north = [(0, anchor_y + upward, anchor_x + offset) for offset in range(across)]
    west = [(1, anchor_x, anchor_y + offset) for offset in range(upward)]
    return south + east + north + west


def pair_tables(former, latter):
    where_latter = {marker: position for position, marker in enumerate(latter)}
    shared = set(former) & set(latter)
    outer_a = [position for position, marker in enumerate(former) if marker not in shared]
    inner_a = [position for position, marker in enumerate(former) if marker in shared]
    inner_b = [where_latter[former[position]] for position in inner_a]
    outer_b = [position for position, marker in enumerate(latter) if marker not in shared]
    joined = [former[position] for position in outer_a] + [latter[position] for position in outer_b]
    tables = (np.array(outer_a), np.array(inner_a), np.array(outer_b), np.array(inner_b))
    return (tables, joined)


def level_tables(points):
    offsets = [(0, points), (points, 0), (0, 2 * points), (2 * points, 0)]

    def labels_at(section, anchor_x, anchor_y):
        if section == 0:
            return box_labels(anchor_x, anchor_y, points, points)
        shift_x, shift_y = offsets[section - 1]
        former = labels_at(section - 1, anchor_x, anchor_y)
        latter = labels_at(section - 1, anchor_x + shift_x, anchor_y + shift_y)
        return pair_tables(former, latter)[1]

    sections = []
    for section in range(1, 5):
        shift_x, shift_y = offsets[section - 1]
        sections.append(
            pair_tables(labels_at(section - 1, 0, 0), labels_at(section - 1, shift_x, shift_y))[0]
        )
    return sections


def fine_tables(points):
    halved = points // 2
    left_tab, left_join = pair_tables(
        box_labels(0, 0, halved, halved), box_labels(0, halved, halved, halved)
    )
    right_tab, right_join = pair_tables(
        box_labels(halved, 0, halved, halved), box_labels(halved, halved, halved, halved)
    )
    whole_tab, whole_join = pair_tables(left_join, right_join)
    where_whole = {marker: position for position, marker in enumerate(whole_join)}
    order = np.array([where_whole[marker] for marker in box_labels(0, 0, points, points)])
    return (left_tab, right_tab, whole_tab, order)


def pick(block, index, axis):
    index = np.asarray(index)
    cuts = [0] + [k for k in range(1, len(index)) if index[k] != index[k - 1] + 1] + [len(index)]
    pieces = []
    for low, high in zip(cuts[:-1], cuts[1:]):
        pieces.append(
            lax.slice_in_dim(block, int(index[low]), int(index[high - 1]) + 1, axis=axis)
        )
    return pieces[0] if len(pieces) == 1 else jnp.concatenate(pieces, axis=axis)


def take(box, rows, cols):
    out = []
    for part in box:
        if rows is not None:
            part = pick(part, rows, 0)
        if cols is not None:
            part = pick(part, cols, 1)
        out.append(part)
    return tuple(out)


def halves(stacked):
    size = stacked.shape[0] // 2
    return stacked[:size], stacked[size:]


def stack(box):
    return jnp.concatenate([box[0], box[1]], axis=0)


def embed(box):
    upper = jnp.concatenate([box[0], -box[1]], axis=1)
    lower = jnp.concatenate([box[1], box[0]], axis=1)
    return jnp.concatenate([upper, lower], axis=0)


def dot(left, right):
    return jnp.dot(left, right, preferred_element_type=jnp.float32)


def split(block):
    high = block.astype(jnp.bfloat16)
    low = (block - high.astype(jnp.float32)).astype(jnp.bfloat16)
    return high, low


def fine_dot(left, right):
    return dot(left[0], right[0]) + (dot(left[0], right[1]) + dot(left[1], right[0]))


def product(left, right):
    return fine_dot(split(embed(left)), split(right))


def unit(size):
    rows = lax.broadcasted_iota(jnp.int32, (2 * size, size), 0)
    cols = lax.broadcasted_iota(jnp.int32, (2 * size, size), 1)
    return jnp.where(rows == cols, 1.0, 0.0).astype(jnp.float32)


def total(block):
    return jnp.sum(jnp.sum(block, axis=0, keepdims=True), axis=1, keepdims=True)[0, 0]


def peak(block):
    return jnp.max(jnp.max(block, axis=0, keepdims=True), axis=1, keepdims=True)[0, 0]


def invert(systems, scratch):
    size = systems[0].shape[1]
    one = unit(size)
    narrow = jnp.bfloat16
    count = len(systems)
    exact = []
    worst = None
    for k, p in enumerate(systems):
        x_ref, r_ref = scratch[k]
        first = one + p
        p_embed = embed(halves(p)).astype(narrow)
        square = dot(p_embed, p.astype(narrow))
        square_embed = embed(halves(square)).astype(narrow)
        second = first + dot(embed(halves(first)).astype(narrow), square.astype(narrow))
        fourth = dot(square_embed, square.astype(narrow))
        x = second + dot(embed(halves(second)).astype(narrow), fourth.astype(narrow))
        a = one - p
        a_split = split(embed(halves(a)))
        r = one - fine_dot(a_split, split(x))
        x_ref[...] = x
        r_ref[...] = r
        norm = total(r * r)
        worst = norm if worst is None else jnp.maximum(worst, norm)
        exact.append((a, a_split))

    def restart():
        norm = jnp.float32(0.0)
        for k in range(count):
            a, a_split = exact[k]
            x_ref, r_ref = scratch[k]
            full = jnp.abs(embed(halves(a)))
            scale = peak(jnp.sum(full, axis=0, keepdims=True)) * peak(
                jnp.sum(full, axis=1, keepdims=True)
            )
            real, imaginary = halves(a)
            x = jnp.concatenate([real.T, -imaginary.T], axis=0) / scale
            r = one - fine_dot(a_split, split(x))
            x_ref[...] = x
            r_ref[...] = r
            norm = jnp.maximum(norm, total(r * r))
        return norm

    worst = lax.cond(worst < 0.25, lambda: worst, restart)

    def unfinished(state):
        return jnp.logical_and(state[0] > 1e-5, state[1] < 200)

    def improve(state):
        norm = jnp.float32(0.0)
        for k in range(count):
            x_ref, r_ref = scratch[k]
            x = x_ref[...]
            x = x + product(halves(x), r_ref[...])
            r = one - fine_dot(exact[k][1], split(x))
            x_ref[...] = x
            r_ref[...] = r
            norm = jnp.maximum(norm, total(r * r))
        return norm, state[1] + 1

    lax.while_loop(unfinished, improve, (worst, jnp.int32(0)))
    return [x_ref[...] + product(halves(x_ref[...]), r_ref[...]) for x_ref, r_ref in scratch[:count]]


def prepare(former, latter, tables):
    outer_a, inner_a, outer_b, inner_b = tables
    size = len(inner_a)
    from_former = take(former, inner_a, np.concatenate([inner_a, outer_a]))
    reflected = product(take(latter, inner_b, inner_b), stack(from_former))
    right_side = jnp.concatenate(
        [reflected[:, size:], -stack(take(latter, inner_b, outer_b))], axis=1
    )
    return reflected[:, :size], right_side


def finish(former, latter, tables, inverse, right_side):
    outer_a, inner_a, outer_b, inner_b = tables
    size_former, size_latter = len(outer_a), len(outer_b)
    solved = product(halves(inverse), right_side)
    rows = np.concatenate([outer_a, inner_a])
    passed = product(take(former, rows, inner_a), solved)
    upper, traces = [], []
    for part, own in zip(halves(passed), take(former, rows, outer_a)):
        wide = jnp.concatenate([own, jnp.zeros((len(rows), size_latter), jnp.float32)], axis=1)
        part = part + wide
        upper.append(part[:size_former])
        traces.append(part[size_former:])
    coupled = product(take(latter, outer_b, inner_b), stack(traces))
    merged = []
    for high, part, own in zip(upper, halves(coupled), take(latter, outer_b, outer_b)):
        wide = jnp.concatenate([jnp.zeros((size_latter, size_former), jnp.float32), own], axis=1)
        merged.append(jnp.concatenate([high, wide - part], axis=0))
    return tuple(merged)


def merge_pair(former, latter, tables, scratch):
    system, right_side = prepare(former, latter, tables)
    (inverse,) = invert([system], [scratch])
    return finish(former, latter, tables, inverse, right_side)


def sides(own_ref, partner_ref, swapped):
    former, latter = [], []
    for part in range(2):
        own, other = own_ref[part], partner_ref[part]
        former.append(jnp.where(swapped, other, own))
        latter.append(jnp.where(swapped, own, other))
    return tuple(former), tuple(latter)


def box_kernel(fine_set, flag_ref, coarse_ref, fine_ref, out_ref, *scratch):
    left_tab, right_tab, whole_tab, order = fine_set
    pairs = [scratch[0:2], scratch[2:4], scratch[4:6]]

    @pl.when(flag_ref[0, 0] > 0)
    def _():
        pieces = [(fine_ref[k, 0], fine_ref[k, 1]) for k in range(4)]
        left_system, left_side = prepare(pieces[0], pieces[1], left_tab)
        right_system, right_side = prepare(pieces[2], pieces[3], right_tab)
        left_inverse, right_inverse = invert([left_system, right_system], pairs)
        left_map = finish(pieces[0], pieces[1], left_tab, left_inverse, left_side)
        right_map = finish(pieces[2], pieces[3], right_tab, right_inverse, right_side)
        whole = take(merge_pair(left_map, right_map, whole_tab, pairs[2]), order, order)
        out_ref[0] = whole[0]
        out_ref[1] = whole[1]

    @pl.when(flag_ref[0, 0] <= 0)
    def _():
        out_ref[...] = coarse_ref[...]


def pair_kernel(tables, place_ref, own_ref, partner_ref, out_ref, *scratch):
    former, latter = sides(own_ref, partner_ref, place_ref[0] > 0)
    merged = merge_pair(former, latter, tables, scratch)
    out_ref[0] = merged[0]
    out_ref[1] = merged[1]


def half_kernel(tables, next_tables, place_ref, own_ref, partner_ref, send_ref, inner_ref, rows_ref, work_ref, *scratch):
    former, latter = sides(own_ref, partner_ref, place_ref[0] > 0)
    merged = merge_pair(former, latter, tables, scratch)
    outer_a, inner_a, outer_b, inner_b = next_tables
    latter_side = place_ref[1] > 0
    size = len(inner_a)
    tile = rows_ref.shape[1]
    near = np.concatenate([inner_a, outer_a])
    far = np.concatenate([inner_b, outer_b])
    for part in range(2):
        chosen = jnp.where(
            latter_side,
            pick(pick(merged[part], far, 0), far, 1),
            pick(pick(merged[part], near, 0), near, 1),
        )
        inner_ref[part] = chosen[:size]
        work_ref[part] = chosen[size:]
        rows_ref[part] = work_ref[part, pl.ds(pl.multiple_of(place_ref[2] * tile, tile), tile), :]
        send_ref[part, :, :size] = chosen[:size, :size]
        send_ref[part, :, size:] = inner_ref[
            part, :, pl.ds(pl.multiple_of(size + place_ref[3] * tile, 128), tile)
        ]


def tile_kernel(place_ref, inner_ref, received_ref, rows_ref, out_ref, *scratch):
    latter_side = place_ref[1] > 0
    latter_tile = place_ref[4] > 0
    size = inner_ref.shape[1]
    tile = rows_ref.shape[1]
    columns = pl.ds(pl.multiple_of(size + place_ref[3] * tile, 128), tile)
    own_inner = [inner_ref[part, :, :size] for part in range(2)]
    got_inner = [received_ref[part, :, :size] for part in range(2)]
    former = [jnp.where(latter_side, got_inner[k], own_inner[k]) for k in range(2)]
    latter = [jnp.where(latter_side, own_inner[k], got_inner[k]) for k in range(2)]
    same = latter_side == latter_tile
    outward = [
        jnp.where(same, inner_ref[k, :, columns], received_ref[k, :, size:]) for k in range(2)
    ]
    reflected = product(latter, jnp.concatenate([stack(former), stack(outward)], axis=1))
    (inverse,) = invert([reflected[:, :size]], [scratch])
    right_side = jnp.where(latter_tile, -stack(outward), reflected[:, size:])
    solved = product(halves(inverse), right_side)
    traces = product(former, solved) + jnp.where(latter_tile, 0.0, stack(outward))
    applied = jnp.where(latter_side, -traces, solved)
    coupling = [rows_ref[k, :, :size] for k in range(2)]
    through = halves(product(coupling, applied))
    for k in range(2):
        out_ref[k] = through[k] + jnp.where(same, rows_ref[k, :, columns], 0.0)


def work(*sizes):
    return [pltpu.VMEM((2 * size, size), jnp.float32) for size in sizes for _ in range(2)]


def call(kernel, shapes, scratch, place, *blocks):
    vmem = pl.BlockSpec(memory_space=pltpu.VMEM)
    outs = [jax.ShapeDtypeStruct(shape, jnp.float32) for shape in shapes]
    single = len(outs) == 1
    return pl.pallas_call(
        kernel,
        out_shape=outs[0] if single else tuple(outs),
        in_specs=[pl.BlockSpec(memory_space=pltpu.SMEM)] + [vmem] * len(blocks),
        out_specs=vmem if single else tuple([vmem] * len(outs)),
        scratch_shapes=scratch,
        compiler_params=pltpu.CompilerParams(vmem_limit_bytes=48 * 1024 * 1024),
    )(place, *blocks)


def body(coarse_map, fine_maps, pml_flag):
    points = coarse_map.shape[-1] // 4
    fine_set = fine_tables(points)
    sections = level_tables(points)
    inner = [len(section[1]) for section in sections]
    width = [len(section[0]) + len(section[2]) for section in sections]
    tile = 4 * points
    gx_index = lax.axis_index("gx")
    gy_index = lax.axis_index("gy")

    def place(swapped):
        return jnp.stack(
            [
                swapped,
                gx_index // 2 % 2,
                gx_index % 2,
                gy_index % 2,
                gy_index // 2 % 2,
            ]
        ).astype(jnp.int32)

    boxed = call(
        functools.partial(box_kernel, fine_set),
        [coarse_map.shape[2:]],
        work(points // 2, points // 2, points),
        pml_flag,
        coarse_map[0, 0],
        fine_maps[0, 0],
    )
    one = call(
        functools.partial(pair_kernel, sections[0]),
        [(2, width[0], width[0])],
        work(inner[0]),
        place(gy_index % 2),
        boxed,
        partner(boxed, "gy", 0),
    )
    two = call(
        functools.partial(pair_kernel, sections[1]),
        [(2, width[1], width[1])],
        work(inner[1]),
        place(gx_index % 2),
        one,
        partner(one, "gx", 0),
    )
    sent, own_inner, own_rows = call(
        functools.partial(half_kernel, sections[2], sections[3]),
        [(2, inner[3], inner[3] + tile), (2, inner[3], width[2]), (2, tile, width[2])],
        [pltpu.VMEM((2, width[2] - inner[3], width[2]), jnp.float32)] + work(inner[2]),
        place(gy_index // 2 % 2),
        two,
        partner(two, "gy", 1),
    )
    return call(
        tile_kernel,
        [(2, tile, tile)],
        work(inner[3]),
        place(gx_index // 2 % 2),
        own_inner,
        partner(sent, "gx", 1),
        own_rows,
    )


def solution(mesh):
    placed = (P("gx", "gy", None, None, None), P("gx", "gy", None, None, None, None), P("gx", "gy"))
    return jax.shard_map(
        body, mesh=mesh, in_specs=placed, out_specs=P(None, "gx", "gy"), check_vma=False
    )
```

```python
import functools
import jax
import jax.numpy as jnp
import numpy as np
from jax import lax
from jax.experimental import pallas as pl
from jax.experimental.pallas import tpu as pltpu
from jax.sharding import PartitionSpec as P

def partner(block, axis, stride):
    count = lax.axis_size(axis)
    route = []
    for low in range(count):
        high = low | 1 << stride
        if high != low and high < count:
            route += [(low, high), (high, low)]
    return lax.ppermute(block, axis, route)


def box_labels(anchor_x, anchor_y, across, upward):
    south = [(0, anchor_y, anchor_x + offset) for offset in range(across)]
    east = [(1, anchor_x + across, anchor_y + offset) for offset in range(upward)]
    north = [(0, anchor_y + upward, anchor_x + offset) for offset in range(across)]
    west = [(1, anchor_x, anchor_y + offset) for offset in range(upward)]
    return south + east + north + west


def pair_tables(former, latter):
    where_latter = {marker: position for position, marker in enumerate(latter)}
    shared = set(former) & set(latter)
    outer_a = [position for position, marker in enumerate(former) if marker not in shared]
    inner_a = [position for position, marker in enumerate(former) if marker in shared]
    inner_b = [where_latter[former[position]] for position in inner_a]
    outer_b = [position for position, marker in enumerate(latter) if marker not in shared]
    joined = [former[position] for position in outer_a] + [latter[position] for position in outer_b]
    tables = (np.array(outer_a), np.array(inner_a), np.array(outer_b), np.array(inner_b))
    return (tables, joined)


def level_tables(points):
    offsets = [(0, points), (points, 0), (0, 2 * points), (2 * points, 0)]

    def labels_at(section, anchor_x, anchor_y):
        if section == 0:
            return box_labels(anchor_x, anchor_y, points, points)
        shift_x, shift_y = offsets[section - 1]
        former = labels_at(section - 1, anchor_x, anchor_y)
        latter = labels_at(section - 1, anchor_x + shift_x, anchor_y + shift_y)
        return pair_tables(former, latter)[1]

    sections = []
    for section in range(1, 5):
        shift_x, shift_y = offsets[section - 1]
        sections.append(
            pair_tables(labels_at(section - 1, 0, 0), labels_at(section - 1, shift_x, shift_y))[0]
        )
    return sections


def fine_tables(points):
    halved = points // 2
    left_tab, left_join = pair_tables(
        box_labels(0, 0, halved, halved), box_labels(0, halved, halved, halved)
    )
    right_tab, right_join = pair_tables(
        box_labels(halved, 0, halved, halved), box_labels(halved, halved, halved, halved)
    )
    whole_tab, whole_join = pair_tables(left_join, right_join)
    where_whole = {marker: position for position, marker in enumerate(whole_join)}
    order = np.array([where_whole[marker] for marker in box_labels(0, 0, points, points)])
    return (left_tab, right_tab, whole_tab, order)


def pick(block, index, axis):
    index = np.asarray(index)
    cuts = [0] + [k for k in range(1, len(index)) if index[k] != index[k - 1] + 1] + [len(index)]
    pieces = []
    for low, high in zip(cuts[:-1], cuts[1:]):
        pieces.append(
            lax.slice_in_dim(block, int(index[low]), int(index[high - 1]) + 1, axis=axis)
        )
    return pieces[0] if len(pieces) == 1 else jnp.concatenate(pieces, axis=axis)


def take(box, rows, cols):
    out = []
    for part in box:
        if rows is not None:
            part = pick(part, rows, 0)
        if cols is not None:
            part = pick(part, cols, 1)
        out.append(part)
    return tuple(out)


def halves(stacked):
    size = stacked.shape[0] // 2
    return stacked[:size], stacked[size:]


def stack(box):
    return jnp.concatenate([box[0], box[1]], axis=0)


def embed(box):
    upper = jnp.concatenate([box[0], -box[1]], axis=1)
    lower = jnp.concatenate([box[1], box[0]], axis=1)
    return jnp.concatenate([upper, lower], axis=0)


def dot(left, right):
    return jnp.dot(left, right, preferred_element_type=jnp.float32)


def split(block):
    high = block.astype(jnp.bfloat16)
    low = (block - high.astype(jnp.float32)).astype(jnp.bfloat16)
    return high, low


def fine_dot(left, right):
    return dot(left[0], right[0]) + (dot(left[0], right[1]) + dot(left[1], right[0]))


def product(left, right):
    return fine_dot(split(embed(left)), split(right))


def unit(size):
    rows = lax.broadcasted_iota(jnp.int32, (2 * size, size), 0)
    cols = lax.broadcasted_iota(jnp.int32, (2 * size, size), 1)
    return jnp.where(rows == cols, 1.0, 0.0).astype(jnp.float32)


def total(block):
    return jnp.sum(jnp.sum(block, axis=0, keepdims=True), axis=1, keepdims=True)[0, 0]


def peak(block):
    return jnp.max(jnp.max(block, axis=0, keepdims=True), axis=1, keepdims=True)[0, 0]


def invert(systems, scratch):
    size = systems[0].shape[1]
    one = unit(size)
    narrow = jnp.bfloat16
    count = len(systems)
    exact = []
    worst = None
    for k, p in enumerate(systems):
        x_ref, r_ref = scratch[k]
        first = one + p
        p_embed = embed(halves(p)).astype(narrow)
        square = dot(p_embed, p.astype(narrow))
        square_embed = embed(halves(square)).astype(narrow)
        second = first + dot(embed(halves(first)).astype(narrow), square.astype(narrow))
        fourth = dot(square_embed, square.astype(narrow))
        x = second + dot(embed(halves(second)).astype(narrow), fourth.astype(narrow))
        a = one - p
        a_split = split(embed(halves(a)))
        r = one - fine_dot(a_split, split(x))
        x_ref[...] = x
        r_ref[...] = r
        norm = total(r * r)
        worst = norm if worst is None else jnp.maximum(worst, norm)
        exact.append((a, a_split))

    def restart():
        norm = jnp.float32(0.0)
        for k in range(count):
            a, a_split = exact[k]
            x_ref, r_ref = scratch[k]
            full = jnp.abs(embed(halves(a)))
            scale = peak(jnp.sum(full, axis=0, keepdims=True)) * peak(
                jnp.sum(full, axis=1, keepdims=True)
            )
            real, imaginary = halves(a)
            x = jnp.concatenate([real.T, -imaginary.T], axis=0) / scale
            r = one - fine_dot(a_split, split(x))
            x_ref[...] = x
            r_ref[...] = r
            norm = jnp.maximum(norm, total(r * r))
        return norm

    worst = lax.cond(worst < 0.25, lambda: worst, restart)

    def unfinished(state):
        return jnp.logical_and(state[0] > 1e-5, state[1] < 200)

    def improve(state):
        norm = jnp.float32(0.0)
        for k in range(count):
            x_ref, r_ref = scratch[k]
            x = x_ref[...]
            x = x + product(halves(x), r_ref[...])
            r = one - fine_dot(exact[k][1], split(x))
            x_ref[...] = x
            r_ref[...] = r
            norm = jnp.maximum(norm, total(r * r))
        return norm, state[1] + 1

    lax.while_loop(unfinished, improve, (worst, jnp.int32(0)))
    return [x_ref[...] + product(halves(x_ref[...]), r_ref[...]) for x_ref, r_ref in scratch[:count]]


def prepare(former, latter, tables):
    outer_a, inner_a, outer_b, inner_b = tables
    size = len(inner_a)
    from_former = take(former, inner_a, np.concatenate([inner_a, outer_a]))
    reflected = product(take(latter, inner_b, inner_b), stack(from_former))
    right_side = jnp.concatenate(
        [reflected[:, size:], -stack(take(latter, inner_b, outer_b))], axis=1
    )
    return reflected[:, :size], right_side


def finish(former, latter, tables, inverse, right_side):
    outer_a, inner_a, outer_b, inner_b = tables
    size_former, size_latter = len(outer_a), len(outer_b)
    solved = product(halves(inverse), right_side)
    rows = np.concatenate([outer_a, inner_a])
    passed = product(take(former, rows, inner_a), solved)
    upper, traces = [], []
    for part, own in zip(halves(passed), take(former, rows, outer_a)):
        wide = jnp.concatenate([own, jnp.zeros((len(rows), size_latter), jnp.float32)], axis=1)
        part = part + wide
        upper.append(part[:size_former])
        traces.append(part[size_former:])
    coupled = product(take(latter, outer_b, inner_b), stack(traces))
    merged = []
    for high, part, own in zip(upper, halves(coupled), take(latter, outer_b, outer_b)):
        wide = jnp.concatenate([jnp.zeros((size_latter, size_former), jnp.float32), own], axis=1)
        merged.append(jnp.concatenate([high, wide - part], axis=0))
    return tuple(merged)


def merge_pair(former, latter, tables, scratch):
    system, right_side = prepare(former, latter, tables)
    (inverse,) = invert([system], [scratch])
    return finish(former, latter, tables, inverse, right_side)


def sides(own_ref, partner_ref, swapped):
    former, latter = [], []
    for part in range(2):
        own, other = own_ref[part], partner_ref[part]
        former.append(jnp.where(swapped, other, own))
        latter.append(jnp.where(swapped, own, other))
    return tuple(former), tuple(latter)


def box_kernel(fine_set, flag_ref, coarse_ref, fine_ref, out_ref, *scratch):
    left_tab, right_tab, whole_tab, order = fine_set
    pairs = [scratch[0:2], scratch[2:4], scratch[4:6]]

    @pl.when(flag_ref[0, 0] > 0)
    def _():
        pieces = [(fine_ref[k, 0], fine_ref[k, 1]) for k in range(4)]
        left_system, left_side = prepare(pieces[0], pieces[1], left_tab)
        right_system, right_side = prepare(pieces[2], pieces[3], right_tab)
        left_inverse, right_inverse = invert([left_system, right_system], pairs)
        left_map = finish(pieces[0], pieces[1], left_tab, left_inverse, left_side)
        right_map = finish(pieces[2], pieces[3], right_tab, right_inverse, right_side)
        whole = take(merge_pair(left_map, right_map, whole_tab, pairs[2]), order, order)
        out_ref[0] = whole[0]
        out_ref[1] = whole[1]

    @pl.when(flag_ref[0, 0] <= 0)
    def _():
        out_ref[...] = coarse_ref[...]


def pair_kernel(tables, place_ref, own_ref, partner_ref, out_ref, *scratch):
    former, latter = sides(own_ref, partner_ref, place_ref[0] > 0)
    merged = merge_pair(former, latter, tables, scratch)
    out_ref[0] = merged[0]
    out_ref[1] = merged[1]


def half_kernel(tables, next_tables, place_ref, own_ref, partner_ref, face_ref, outward_ref, rows_ref, *scratch):
    former, latter = sides(own_ref, partner_ref, place_ref[0] > 0)
    merged = merge_pair(former, latter, tables, scratch)
    outer_a, inner_a, outer_b, inner_b = next_tables
    latter_side = place_ref[1] > 0
    second_rows = place_ref[2] > 0
    second_cols = place_ref[3] > 0
    size = len(inner_a)
    tile = rows_ref.shape[1]
    near = np.concatenate([inner_a, outer_a])
    far = np.concatenate([inner_b, outer_b])
    for part in range(2):
        chosen = jnp.where(
            latter_side,
            pick(pick(merged[part], far, 0), far, 1),
            pick(pick(merged[part], near, 0), near, 1),
        )
        low, high = size + tile, size + 2 * tile
        cols = jnp.where(second_cols, chosen[:, low:high], chosen[:, size:low])
        face_ref[part] = chosen[:size, :size]
        outward_ref[part] = cols[:size]
        coupling = chosen[:, :size]
        rows_ref[part, :, :size] = jnp.where(second_rows, coupling[low:high], coupling[size:low])
        rows_ref[part, :, size:] = jnp.where(second_rows, cols[low:high], cols[size:low])


def tile_kernel(place_ref, face_ref, outward_ref, got_face_ref, got_outward_ref, rows_ref, out_ref, *scratch):
    latter_side = place_ref[1] > 0
    latter_tile = place_ref[4] > 0
    size = face_ref.shape[1]
    former = [jnp.where(latter_side, got_face_ref[k], face_ref[k]) for k in range(2)]
    latter = [jnp.where(latter_side, face_ref[k], got_face_ref[k]) for k in range(2)]
    same = latter_side == latter_tile
    outward = stack([jnp.where(same, outward_ref[k], got_outward_ref[k]) for k in range(2)])
    reflected = product(latter, jnp.concatenate([stack(former), outward], axis=1))
    (inverse,) = invert([reflected[:, :size]], [scratch])
    right_side = jnp.where(latter_tile, -outward, reflected[:, size:])
    solved = product(halves(inverse), right_side)
    traces = product(former, solved) + jnp.where(latter_tile, 0.0, outward)
    applied = jnp.where(latter_side, -traces, solved)
    coupling = [rows_ref[k, :, :size] for k in range(2)]
    through = halves(product(coupling, applied))
    for k in range(2):
        out_ref[k] = through[k] + jnp.where(same, rows_ref[k, :, size:], 0.0)


def flipped(index, bit):
    step = 2**bit
    return index + step * (1 - 2 * lax.rem(lax.div(index, step), 2))


def hop(source, target, sems, slot, device):
    return pltpu.make_async_remote_copy(
        src_ref=source,
        dst_ref=target,
        send_sem=sems[0].at[slot],
        recv_sem=sems[1].at[slot],
        device_id=device,
        device_id_type=pl.DeviceIdType.MESH,
    )


def greet(devices):
    barrier = pltpu.get_barrier_semaphore()
    for device in devices:
        pl.semaphore_signal(
            barrier, inc=1, device_id=device, device_id_type=pl.DeviceIdType.MESH
        )
    pl.semaphore_wait(barrier, len(devices))


def swap_kernel(axis, bit, chunks, own_ref, out_ref, far_send, far_recv, near_send, near_recv):
    gx, gy = lax.axis_index("gx"), lax.axis_index("gy")
    peer = (flipped(gx, bit), gy) if axis == "gx" else (gx, flipped(gy, bit))
    sibling = (gx, flipped(gy, 0))
    mine = lax.rem(gy, 2)
    greet([peer, sibling])
    rows = own_ref.shape[1] // chunks
    far, near = (far_send, far_recv), (near_send, near_recv)
    out, relays = [], []
    for k in range(chunks):
        spot = (mine, pl.ds(k * rows, rows))
        copy = hop(own_ref.at[spot], out_ref.at[spot], far, k, peer)
        copy.start()
        out.append(copy)
        relays.append(hop(out_ref.at[spot], out_ref.at[spot], near, k, sibling))
    for k in range(chunks):
        out[k].wait_recv()
        relays[k].start()
    for k in range(chunks):
        relays[k].wait_recv()
    for k in range(chunks):
        out[k].wait_send()
        relays[k].wait_send()


def line_kernel(face_ref, outward_ref, got_face_ref, got_outward_ref, far_send, far_recv, on_send, on_recv, near_send, near_recv):
    gx, gy = lax.axis_index("gx"), lax.axis_index("gy")
    low, second = lax.rem(gx, 2), lax.rem(lax.div(gx, 2), 2)
    middle = low != second
    across = (gx + 1 - 2 * second, gy)
    along = (flipped(gx, 0), gy)
    sibling = (gx, flipped(gy, 0))
    mine = lax.rem(gy, 2)
    group = lax.rem(lax.div(gy, 2), 2)
    gives = group == second
    takes = group != second

    @pl.when(middle)
    def _():
        greet([across, along, sibling])

    @pl.when(jnp.logical_not(middle))
    def _():
        greet([along, sibling])

    rows = outward_ref.shape[1] // 2
    spots = [(part, pl.ds(k * rows, rows)) for part in range(2) for k in range(2)]
    far, on, near = (far_send, far_recv), (on_send, on_recv), (near_send, near_recv)
    face_far = hop(face_ref.at[mine], got_face_ref.at[mine], far, 0, across)
    face_on = hop(got_face_ref.at[mine], got_face_ref.at[mine], on, 0, along)
    face_near = hop(got_face_ref.at[mine], got_face_ref.at[mine], near, 0, sibling)
    cols_far = [
        hop(outward_ref.at[spot], got_outward_ref.at[spot], far, k + 1, across)
        for k, spot in enumerate(spots)
    ]
    cols_on = [
        hop(got_outward_ref.at[spot], got_outward_ref.at[spot], on, k + 1, along)
        for k, spot in enumerate(spots)
    ]

    @pl.when(middle)
    def _():
        face_far.start()

        @pl.when(gives)
        def _():
            for copy in cols_far:
                copy.start()

        face_far.wait_recv()
        face_on.start()
        face_near.start()

        @pl.when(takes)
        def _():
            for first, then in zip(cols_far, cols_on):
                first.wait_recv()
                then.start()
            for then in cols_on:
                then.wait_send()

        @pl.when(gives)
        def _():
            for copy in cols_far:
                copy.wait_send()

        face_far.wait_send()
        face_on.wait_send()

    @pl.when(jnp.logical_not(middle))
    def _():
        face_on.wait_recv()
        face_near.start()

        @pl.when(takes)
        def _():
            for copy in cols_on:
                copy.wait_recv()

    face_near.wait_recv()
    face_near.wait_send()


def exchange(kernel, identity, copies, *blocks):
    vmem = pl.BlockSpec(memory_space=pltpu.VMEM)
    outs = [jax.ShapeDtypeStruct(block.shape, block.dtype) for block in blocks]
    single = len(outs) == 1
    return pl.pallas_call(
        kernel,
        out_shape=outs[0] if single else tuple(outs),
        in_specs=[vmem] * len(blocks),
        out_specs=vmem if single else tuple([vmem] * len(outs)),
        scratch_shapes=[pltpu.SemaphoreType.DMA((count,)) for count in copies for _ in range(2)],
        compiler_params=pltpu.CompilerParams(collective_id=identity, has_side_effects=True),
    )(*blocks)


def swap(block, axis, bit, identity):
    chunks = 4
    return exchange(
        functools.partial(swap_kernel, axis, bit, chunks), identity, (chunks, chunks), block
    )


def work(*sizes):
    return [pltpu.VMEM((2 * size, size), jnp.float32) for size in sizes for _ in range(2)]


def call(kernel, shapes, scratch, place, *blocks):
    vmem = pl.BlockSpec(memory_space=pltpu.VMEM)
    outs = [jax.ShapeDtypeStruct(shape, jnp.float32) for shape in shapes]
    single = len(outs) == 1
    return pl.pallas_call(
        kernel,
        out_shape=outs[0] if single else tuple(outs),
        in_specs=[pl.BlockSpec(memory_space=pltpu.SMEM)] + [vmem] * len(blocks),
        out_specs=vmem if single else tuple([vmem] * len(outs)),
        scratch_shapes=scratch,
        compiler_params=pltpu.CompilerParams(vmem_limit_bytes=48 * 1024 * 1024),
    )(place, *blocks)


def body(coarse_map, fine_maps, pml_flag):
    points = coarse_map.shape[-1] // 4
    fine_set = fine_tables(points)
    sections = level_tables(points)
    inner = [len(section[1]) for section in sections]
    width = [len(section[0]) + len(section[2]) for section in sections]
    tile = 4 * points
    gx_index = lax.axis_index("gx")
    gy_index = lax.axis_index("gy")

    def place(swapped):
        return jnp.stack(
            [
                swapped,
                gx_index // 2 % 2,
                gx_index % 2,
                gy_index % 2,
                gy_index // 2 % 2,
            ]
        ).astype(jnp.int32)

    boxed = call(
        functools.partial(box_kernel, fine_set),
        [coarse_map.shape[2:]],
        work(points // 2, points // 2, points),
        pml_flag,
        coarse_map[0, 0],
        fine_maps[0, 0],
    )
    one = call(
        functools.partial(pair_kernel, sections[0]),
        [(2, width[0], width[0])],
        work(inner[0]),
        place(gy_index % 2),
        boxed,
        partner(boxed, "gy", 0),
    )
    two = call(
        functools.partial(pair_kernel, sections[1]),
        [(2, width[1], width[1])],
        work(inner[1]),
        place(gx_index % 2),
        one,
        swap(one, "gx", 0, 0),
    )
    face, outward, own_rows = call(
        functools.partial(half_kernel, sections[2], sections[3]),
        [(2, inner[3], inner[3]), (2, inner[3], tile), (2, tile, inner[3] + tile)],
        work(inner[2]),
        place(gy_index // 2 % 2),
        two,
        swap(two, "gy", 1, 1),
    )
    got_face, got_outward = exchange(line_kernel, 2, (5, 5, 1), face, outward)
    return call(
        tile_kernel,
        [(2, tile, tile)],
        work(inner[3]),
        place(gx_index // 2 % 2),
        face,
        outward,
        got_face,
        got_outward,
        own_rows,
    )


def solution(mesh):
    placed = (P("gx", "gy", None, None, None), P("gx", "gy", None, None, None, None), P("gx", "gy"))
    return jax.shard_map(
        body, mesh=mesh, in_specs=placed, out_specs=P(None, "gx", "gy"), check_vma=False
    )
```

```python
import functools
import jax
import jax.numpy as jnp
import numpy as np
from jax import lax
from jax.experimental import pallas as pl
from jax.experimental.pallas import tpu as pltpu
from jax.sharding import PartitionSpec as P

def partner(block, axis, stride):
    count = lax.axis_size(axis)
    route = []
    for low in range(count):
        high = low | 1 << stride
        if high != low and high < count:
            route += [(low, high), (high, low)]
    return lax.ppermute(block, axis, route)


def box_labels(anchor_x, anchor_y, across, upward):
    south = [(0, anchor_y, anchor_x + offset) for offset in range(across)]
    east = [(1, anchor_x + across, anchor_y + offset) for offset in range(upward)]
    north = [(0, anchor_y + upward, anchor_x + offset) for offset in range(across)]
    west = [(1, anchor_x, anchor_y + offset) for offset in range(upward)]
    return south + east + north + west


def pair_tables(former, latter):
    where_latter = {marker: position for position, marker in enumerate(latter)}
    shared = set(former) & set(latter)
    outer_a = [position for position, marker in enumerate(former) if marker not in shared]
    inner_a = [position for position, marker in enumerate(former) if marker in shared]
    inner_b = [where_latter[former[position]] for position in inner_a]
    outer_b = [position for position, marker in enumerate(latter) if marker not in shared]
    joined = [former[position] for position in outer_a] + [latter[position] for position in outer_b]
    tables = (np.array(outer_a), np.array(inner_a), np.array(outer_b), np.array(inner_b))
    return (tables, joined)


def level_tables(points):
    offsets = [(0, points), (points, 0), (0, 2 * points), (2 * points, 0)]

    def labels_at(section, anchor_x, anchor_y):
        if section == 0:
            return box_labels(anchor_x, anchor_y, points, points)
        shift_x, shift_y = offsets[section - 1]
        former = labels_at(section - 1, anchor_x, anchor_y)
        latter = labels_at(section - 1, anchor_x + shift_x, anchor_y + shift_y)
        return pair_tables(former, latter)[1]

    sections = []
    for section in range(1, 5):
        shift_x, shift_y = offsets[section - 1]
        sections.append(
            pair_tables(labels_at(section - 1, 0, 0), labels_at(section - 1, shift_x, shift_y))[0]
        )
    return sections


def fine_tables(points):
    halved = points // 2
    left_tab, left_join = pair_tables(
        box_labels(0, 0, halved, halved), box_labels(0, halved, halved, halved)
    )
    right_tab, right_join = pair_tables(
        box_labels(halved, 0, halved, halved), box_labels(halved, halved, halved, halved)
    )
    whole_tab, whole_join = pair_tables(left_join, right_join)
    where_whole = {marker: position for position, marker in enumerate(whole_join)}
    order = np.array([where_whole[marker] for marker in box_labels(0, 0, points, points)])
    return (left_tab, right_tab, whole_tab, order)


def pick(block, index, axis):
    index = np.asarray(index)
    cuts = [0] + [k for k in range(1, len(index)) if index[k] != index[k - 1] + 1] + [len(index)]
    pieces = []
    for low, high in zip(cuts[:-1], cuts[1:]):
        pieces.append(
            lax.slice_in_dim(block, int(index[low]), int(index[high - 1]) + 1, axis=axis)
        )
    return pieces[0] if len(pieces) == 1 else jnp.concatenate(pieces, axis=axis)


def take(box, rows, cols):
    out = []
    for part in box:
        if rows is not None:
            part = pick(part, rows, 0)
        if cols is not None:
            part = pick(part, cols, 1)
        out.append(part)
    return tuple(out)


def halves(stacked):
    size = stacked.shape[0] // 2
    return stacked[:size], stacked[size:]


def stack(box):
    return jnp.concatenate([box[0], box[1]], axis=0)


def embed(box):
    upper = jnp.concatenate([box[0], -box[1]], axis=1)
    lower = jnp.concatenate([box[1], box[0]], axis=1)
    return jnp.concatenate([upper, lower], axis=0)


def dot(left, right):
    return jnp.dot(left, right, preferred_element_type=jnp.float32)


def split(block):
    high = block.astype(jnp.bfloat16)
    low = (block - high.astype(jnp.float32)).astype(jnp.bfloat16)
    return high, low


def fine_dot(left, right):
    return dot(left[0], right[0]) + (dot(left[0], right[1]) + dot(left[1], right[0]))


def product(left, right):
    return fine_dot(split(embed(left)), split(right))


def unit(size):
    rows = lax.broadcasted_iota(jnp.int32, (2 * size, size), 0)
    cols = lax.broadcasted_iota(jnp.int32, (2 * size, size), 1)
    return jnp.where(rows == cols, 1.0, 0.0).astype(jnp.float32)


def total(block):
    return jnp.sum(jnp.sum(block, axis=0, keepdims=True), axis=1, keepdims=True)[0, 0]


def peak(block):
    return jnp.max(jnp.max(block, axis=0, keepdims=True), axis=1, keepdims=True)[0, 0]


def invert(systems, scratch):
    size = systems[0].shape[1]
    one = unit(size)
    narrow = jnp.bfloat16
    count = len(systems)
    exact = []
    worst = None
    for k, p in enumerate(systems):
        x_ref, r_ref = scratch[k]
        first = one + p
        p_embed = embed(halves(p)).astype(narrow)
        square = dot(p_embed, p.astype(narrow))
        square_embed = embed(halves(square)).astype(narrow)
        second = first + dot(embed(halves(first)).astype(narrow), square.astype(narrow))
        fourth = dot(square_embed, square.astype(narrow))
        x = second + dot(embed(halves(second)).astype(narrow), fourth.astype(narrow))
        a = one - p
        a_split = split(embed(halves(a)))
        r = one - fine_dot(a_split, split(x))
        x_ref[...] = x
        r_ref[...] = r
        norm = total(r * r)
        worst = norm if worst is None else jnp.maximum(worst, norm)
        exact.append((a, a_split))

    def restart():
        norm = jnp.float32(0.0)
        for k in range(count):
            a, a_split = exact[k]
            x_ref, r_ref = scratch[k]
            full = jnp.abs(embed(halves(a)))
            scale = peak(jnp.sum(full, axis=0, keepdims=True)) * peak(
                jnp.sum(full, axis=1, keepdims=True)
            )
            real, imaginary = halves(a)
            x = jnp.concatenate([real.T, -imaginary.T], axis=0) / scale
            r = one - fine_dot(a_split, split(x))
            x_ref[...] = x
            r_ref[...] = r
            norm = jnp.maximum(norm, total(r * r))
        return norm

    worst = lax.cond(worst < 0.25, lambda: worst, restart)

    def unfinished(state):
        return jnp.logical_and(state[0] > 1e-5, state[1] < 200)

    def improve(state):
        norm = jnp.float32(0.0)
        for k in range(count):
            x_ref, r_ref = scratch[k]
            x = x_ref[...]
            x = x + product(halves(x), r_ref[...])
            r = one - fine_dot(exact[k][1], split(x))
            x_ref[...] = x
            r_ref[...] = r
            norm = jnp.maximum(norm, total(r * r))
        return norm, state[1] + 1

    lax.while_loop(unfinished, improve, (worst, jnp.int32(0)))
    return [x_ref[...] + product(halves(x_ref[...]), r_ref[...]) for x_ref, r_ref in scratch[:count]]


def prepare(former, latter, tables):
    outer_a, inner_a, outer_b, inner_b = tables
    size = len(inner_a)
    from_former = take(former, inner_a, np.concatenate([inner_a, outer_a]))
    reflected = product(take(latter, inner_b, inner_b), stack(from_former))
    right_side = jnp.concatenate(
        [reflected[:, size:], -stack(take(latter, inner_b, outer_b))], axis=1
    )
    return reflected[:, :size], right_side


def finish(former, latter, tables, inverse, right_side):
    outer_a, inner_a, outer_b, inner_b = tables
    size_former, size_latter = len(outer_a), len(outer_b)
    solved = product(halves(inverse), right_side)
    rows = np.concatenate([outer_a, inner_a])
    passed = product(take(former, rows, inner_a), solved)
    upper, traces = [], []
    for part, own in zip(halves(passed), take(former, rows, outer_a)):
        wide = jnp.concatenate([own, jnp.zeros((len(rows), size_latter), jnp.float32)], axis=1)
        part = part + wide
        upper.append(part[:size_former])
        traces.append(part[size_former:])
    coupled = product(take(latter, outer_b, inner_b), stack(traces))
    merged = []
    for high, part, own in zip(upper, halves(coupled), take(latter, outer_b, outer_b)):
        wide = jnp.concatenate([jnp.zeros((size_latter, size_former), jnp.float32), own], axis=1)
        merged.append(jnp.concatenate([high, wide - part], axis=0))
    return tuple(merged)


def merge_pair(former, latter, tables, scratch):
    system, right_side = prepare(former, latter, tables)
    (inverse,) = invert([system], [scratch])
    return finish(former, latter, tables, inverse, right_side)


def sides(own_ref, partner_ref, swapped):
    former, latter = [], []
    for part in range(2):
        own, other = own_ref[part], partner_ref[part]
        former.append(jnp.where(swapped, other, own))
        latter.append(jnp.where(swapped, own, other))
    return tuple(former), tuple(latter)


def box_kernel(fine_set, flag_ref, coarse_ref, fine_ref, out_ref, *scratch):
    left_tab, right_tab, whole_tab, order = fine_set
    pairs = [scratch[0:2], scratch[2:4], scratch[4:6]]

    @pl.when(flag_ref[0, 0] > 0)
    def _():
        pieces = [(fine_ref[k, 0], fine_ref[k, 1]) for k in range(4)]
        left_system, left_side = prepare(pieces[0], pieces[1], left_tab)
        right_system, right_side = prepare(pieces[2], pieces[3], right_tab)
        left_inverse, right_inverse = invert([left_system, right_system], pairs)
        left_map = finish(pieces[0], pieces[1], left_tab, left_inverse, left_side)
        right_map = finish(pieces[2], pieces[3], right_tab, right_inverse, right_side)
        whole = take(merge_pair(left_map, right_map, whole_tab, pairs[2]), order, order)
        out_ref[0] = whole[0]
        out_ref[1] = whole[1]

    @pl.when(flag_ref[0, 0] <= 0)
    def _():
        out_ref[...] = coarse_ref[...]


def pair_kernel(tables, place_ref, own_ref, partner_ref, out_ref, *scratch):
    former, latter = sides(own_ref, partner_ref, place_ref[0] > 0)
    merged = merge_pair(former, latter, tables, scratch)
    out_ref[0] = merged[0]
    out_ref[1] = merged[1]


def half_kernel(tables, next_tables, place_ref, own_ref, partner_ref, face_ref, outward_ref, rows_ref, *scratch):
    former, latter = sides(own_ref, partner_ref, place_ref[0] > 0)
    merged = merge_pair(former, latter, tables, scratch)
    outer_a, inner_a, outer_b, inner_b = next_tables
    latter_side = place_ref[1] > 0
    second_rows = place_ref[2] > 0
    second_cols = place_ref[3] > 0
    size = len(inner_a)
    tile = rows_ref.shape[1]
    near = np.concatenate([inner_a, outer_a])
    far = np.concatenate([inner_b, outer_b])
    for part in range(2):
        chosen = jnp.where(
            latter_side,
            pick(pick(merged[part], far, 0), far, 1),
            pick(pick(merged[part], near, 0), near, 1),
        )
        low, high = size + tile, size + 2 * tile
        cols = jnp.where(second_cols, chosen[:, low:high], chosen[:, size:low])
        face_ref[part] = chosen[:size, :size]
        outward_ref[part] = cols[:size]
        coupling = chosen[:, :size]
        rows_ref[part, :, :size] = jnp.where(second_rows, coupling[low:high], coupling[size:low])
        rows_ref[part, :, size:] = jnp.where(second_rows, cols[low:high], cols[size:low])


def tile_kernel(place_ref, face_ref, outward_ref, got_face_ref, got_outward_ref, rows_ref, out_ref, *scratch):
    latter_side = place_ref[1] > 0
    latter_tile = place_ref[4] > 0
    size = face_ref.shape[1]
    former = [jnp.where(latter_side, got_face_ref[k], face_ref[k]) for k in range(2)]
    latter = [jnp.where(latter_side, face_ref[k], got_face_ref[k]) for k in range(2)]
    same = latter_side == latter_tile
    outward = stack([jnp.where(same, outward_ref[k], got_outward_ref[k]) for k in range(2)])
    reflected = product(latter, jnp.concatenate([stack(former), outward], axis=1))
    (inverse,) = invert([reflected[:, :size]], [scratch])
    right_side = jnp.where(latter_tile, -outward, reflected[:, size:])
    solved = product(halves(inverse), right_side)
    traces = product(former, solved) + jnp.where(latter_tile, 0.0, outward)
    applied = jnp.where(latter_side, -traces, solved)
    coupling = [rows_ref[k, :, :size] for k in range(2)]
    through = halves(product(coupling, applied))
    for k in range(2):
        out_ref[k] = through[k] + jnp.where(same, rows_ref[k, :, size:], 0.0)


def flipped(index, bit):
    step = 2**bit
    return index + step * (1 - 2 * lax.rem(lax.div(index, step), 2))


def hop(source, target, sems, slot, device):
    return pltpu.make_async_remote_copy(
        src_ref=source,
        dst_ref=target,
        send_sem=sems[0].at[slot],
        recv_sem=sems[1].at[slot],
        device_id=device,
        device_id_type=pl.DeviceIdType.MESH,
    )


def greet(devices):
    barrier = pltpu.get_barrier_semaphore()
    for device in devices:
        pl.semaphore_signal(
            barrier, inc=1, device_id=device, device_id_type=pl.DeviceIdType.MESH
        )
    pl.semaphore_wait(barrier, len(devices))


def swap_kernel(axis, bit, chunks, own_ref, out_ref, far_send, far_recv, near_send, near_recv):
    gx, gy = lax.axis_index("gx"), lax.axis_index("gy")
    peer = (flipped(gx, bit), gy) if axis == "gx" else (gx, flipped(gy, bit))
    sibling = (gx, flipped(gy, 0))
    mine = lax.rem(gy, 2)
    greet([peer, sibling])
    rows = own_ref.shape[1] // chunks
    far, near = (far_send, far_recv), (near_send, near_recv)
    out, relays = [], []
    for k in range(chunks):
        spot = (mine, pl.ds(k * rows, rows))
        copy = hop(own_ref.at[spot], out_ref.at[spot], far, k, peer)
        copy.start()
        out.append(copy)
        relays.append(hop(out_ref.at[spot], out_ref.at[spot], near, k, sibling))
    for k in range(chunks):
        out[k].wait_recv()
        relays[k].start()
    for k in range(chunks):
        relays[k].wait_recv()
    for k in range(chunks):
        out[k].wait_send()
        relays[k].wait_send()


def line_kernel(face_ref, outward_ref, got_face_ref, got_outward_ref, far_send, far_recv, on_send, on_recv, near_send, near_recv):
    gx, gy = lax.axis_index("gx"), lax.axis_index("gy")
    low, second = lax.rem(gx, 2), lax.rem(lax.div(gx, 2), 2)
    middle = low != second
    across = (gx + 1 - 2 * second, gy)
    along = (flipped(gx, 0), gy)
    sibling = (gx, flipped(gy, 0))
    mine = lax.rem(gy, 2)
    group = lax.rem(lax.div(gy, 2), 2)
    gives = group == second
    takes = group != second

    @pl.when(middle)
    def _():
        greet([across, along, sibling])

    @pl.when(jnp.logical_not(middle))
    def _():
        greet([along, sibling])

    rows = outward_ref.shape[1] // 2
    spots = [(part, pl.ds(k * rows, rows)) for part in range(2) for k in range(2)]
    far, on, near = (far_send, far_recv), (on_send, on_recv), (near_send, near_recv)
    face_far = hop(face_ref.at[mine], got_face_ref.at[mine], far, 0, across)
    face_on = hop(got_face_ref.at[mine], got_face_ref.at[mine], on, 0, along)
    face_near = hop(got_face_ref.at[mine], got_face_ref.at[mine], near, 0, sibling)
    cols_far = [
        hop(outward_ref.at[spot], got_outward_ref.at[spot], far, k + 1, across)
        for k, spot in enumerate(spots)
    ]
    cols_on = [
        hop(got_outward_ref.at[spot], got_outward_ref.at[spot], on, k + 1, along)
        for k, spot in enumerate(spots)
    ]

    @pl.when(middle)
    def _():
        face_far.start()

        @pl.when(gives)
        def _():
            for copy in cols_far:
                copy.start()

        face_far.wait_recv()
        face_on.start()
        face_near.start()

        @pl.when(takes)
        def _():
            for first, then in zip(cols_far, cols_on):
                first.wait_recv()
                then.start()
            for then in cols_on:
                then.wait_send()

        @pl.when(gives)
        def _():
            for copy in cols_far:
                copy.wait_send()

        face_far.wait_send()
        face_on.wait_send()

    @pl.when(jnp.logical_not(middle))
    def _():
        face_on.wait_recv()
        face_near.start()

        @pl.when(takes)
        def _():
            for copy in cols_on:
                copy.wait_recv()

    face_near.wait_recv()
    face_near.wait_send()


def exchange(kernel, identity, copies, *blocks):
    vmem = pl.BlockSpec(memory_space=pltpu.VMEM)
    outs = [jax.ShapeDtypeStruct(block.shape, block.dtype) for block in blocks]
    single = len(outs) == 1
    return pl.pallas_call(
        kernel,
        out_shape=outs[0] if single else tuple(outs),
        in_specs=[vmem] * len(blocks),
        out_specs=vmem if single else tuple([vmem] * len(outs)),
        scratch_shapes=[pltpu.SemaphoreType.DMA((count,)) for count in copies for _ in range(2)],
        compiler_params=pltpu.CompilerParams(collective_id=identity, has_side_effects=True, vmem_limit_bytes=4 * 1024 * 1024),
    )(*blocks)


def swap(block, axis, bit, identity):
    chunks = 4
    return exchange(
        functools.partial(swap_kernel, axis, bit, chunks), identity, (chunks, chunks), block
    )


def work(*sizes):
    return [pltpu.VMEM((2 * size, size), jnp.float32) for size in sizes for _ in range(2)]


def call(kernel, shapes, scratch, place, *blocks):
    vmem = pl.BlockSpec(memory_space=pltpu.VMEM)
    outs = [jax.ShapeDtypeStruct(shape, jnp.float32) for shape in shapes]
    single = len(outs) == 1
    return pl.pallas_call(
        kernel,
        out_shape=outs[0] if single else tuple(outs),
        in_specs=[pl.BlockSpec(memory_space=pltpu.SMEM)] + [vmem] * len(blocks),
        out_specs=vmem if single else tuple([vmem] * len(outs)),
        scratch_shapes=scratch,
        compiler_params=pltpu.CompilerParams(vmem_limit_bytes=12 * 1024 * 1024),
    )(place, *blocks)


def body(coarse_map, fine_maps, pml_flag):
    points = coarse_map.shape[-1] // 4
    fine_set = fine_tables(points)
    sections = level_tables(points)
    inner = [len(section[1]) for section in sections]
    width = [len(section[0]) + len(section[2]) for section in sections]
    tile = 4 * points
    gx_index = lax.axis_index("gx")
    gy_index = lax.axis_index("gy")

    def place(swapped):
        return jnp.stack(
            [
                swapped,
                gx_index // 2 % 2,
                gx_index % 2,
                gy_index % 2,
                gy_index // 2 % 2,
            ]
        ).astype(jnp.int32)

    boxed = call(
        functools.partial(box_kernel, fine_set),
        [coarse_map.shape[2:]],
        work(points // 2, points // 2, points),
        pml_flag,
        coarse_map[0, 0],
        fine_maps[0, 0],
    )
    one = call(
        functools.partial(pair_kernel, sections[0]),
        [(2, width[0], width[0])],
        work(inner[0]),
        place(gy_index % 2),
        boxed,
        partner(boxed, "gy", 0),
    )
    two = call(
        functools.partial(pair_kernel, sections[1]),
        [(2, width[1], width[1])],
        work(inner[1]),
        place(gx_index % 2),
        one,
        swap(one, "gx", 0, 0),
    )
    face, outward, own_rows = call(
        functools.partial(half_kernel, sections[2], sections[3]),
        [(2, inner[3], inner[3]), (2, inner[3], tile), (2, tile, inner[3] + tile)],
        work(inner[2]),
        place(gy_index // 2 % 2),
        two,
        swap(two, "gy", 1, 1),
    )
    got_face, got_outward = exchange(line_kernel, 2, (5, 5, 1), face, outward)
    return call(
        tile_kernel,
        [(2, tile, tile)],
        work(inner[3]),
        place(gx_index // 2 % 2),
        face,
        outward,
        got_face,
        got_outward,
        own_rows,
    )


def solution(mesh):
    placed = (P("gx", "gy", None, None, None), P("gx", "gy", None, None, None, None), P("gx", "gy"))
    return jax.shard_map(
        body, mesh=mesh, in_specs=placed, out_specs=P(None, "gx", "gy"), check_vma=False
    )
```

```python
import functools
import jax
import jax.numpy as jnp
import numpy as np
from jax import lax
from jax.experimental import pallas as pl
from jax.experimental.pallas import tpu as pltpu
from jax.sharding import PartitionSpec as P

def partner(block, axis, stride):
    count = lax.axis_size(axis)
    route = []
    for low in range(count):
        high = low | 1 << stride
        if high != low and high < count:
            route += [(low, high), (high, low)]
    return lax.ppermute(block, axis, route)


def box_labels(anchor_x, anchor_y, across, upward):
    south = [(0, anchor_y, anchor_x + offset) for offset in range(across)]
    east = [(1, anchor_x + across, anchor_y + offset) for offset in range(upward)]
    north = [(0, anchor_y + upward, anchor_x + offset) for offset in range(across)]
    west = [(1, anchor_x, anchor_y + offset) for offset in range(upward)]
    return south + east + north + west


def pair_tables(former, latter):
    where_latter = {marker: position for position, marker in enumerate(latter)}
    shared = set(former) & set(latter)
    outer_a = [position for position, marker in enumerate(former) if marker not in shared]
    inner_a = [position for position, marker in enumerate(former) if marker in shared]
    inner_b = [where_latter[former[position]] for position in inner_a]
    outer_b = [position for position, marker in enumerate(latter) if marker not in shared]
    joined = [former[position] for position in outer_a] + [latter[position] for position in outer_b]
    tables = (np.array(outer_a), np.array(inner_a), np.array(outer_b), np.array(inner_b))
    return (tables, joined)


def level_tables(points):
    offsets = [(0, points), (points, 0), (0, 2 * points), (2 * points, 0)]

    def labels_at(section, anchor_x, anchor_y):
        if section == 0:
            return box_labels(anchor_x, anchor_y, points, points)
        shift_x, shift_y = offsets[section - 1]
        former = labels_at(section - 1, anchor_x, anchor_y)
        latter = labels_at(section - 1, anchor_x + shift_x, anchor_y + shift_y)
        return pair_tables(former, latter)[1]

    sections = []
    for section in range(1, 5):
        shift_x, shift_y = offsets[section - 1]
        sections.append(
            pair_tables(labels_at(section - 1, 0, 0), labels_at(section - 1, shift_x, shift_y))[0]
        )
    return sections


def fine_tables(points):
    halved = points // 2
    left_tab, left_join = pair_tables(
        box_labels(0, 0, halved, halved), box_labels(0, halved, halved, halved)
    )
    right_tab, right_join = pair_tables(
        box_labels(halved, 0, halved, halved), box_labels(halved, halved, halved, halved)
    )
    whole_tab, whole_join = pair_tables(left_join, right_join)
    where_whole = {marker: position for position, marker in enumerate(whole_join)}
    order = np.array([where_whole[marker] for marker in box_labels(0, 0, points, points)])
    return (left_tab, right_tab, whole_tab, order)


def pick(block, index, axis):
    index = np.asarray(index)
    cuts = [0] + [k for k in range(1, len(index)) if index[k] != index[k - 1] + 1] + [len(index)]
    pieces = []
    for low, high in zip(cuts[:-1], cuts[1:]):
        pieces.append(
            lax.slice_in_dim(block, int(index[low]), int(index[high - 1]) + 1, axis=axis)
        )
    return pieces[0] if len(pieces) == 1 else jnp.concatenate(pieces, axis=axis)


def take(box, rows, cols):
    out = []
    for part in box:
        if rows is not None:
            part = pick(part, rows, 0)
        if cols is not None:
            part = pick(part, cols, 1)
        out.append(part)
    return tuple(out)


def halves(stacked):
    size = stacked.shape[0] // 2
    return stacked[:size], stacked[size:]


def stack(box):
    return jnp.concatenate([box[0], box[1]], axis=0)


def embed(box):
    upper = jnp.concatenate([box[0], -box[1]], axis=1)
    lower = jnp.concatenate([box[1], box[0]], axis=1)
    return jnp.concatenate([upper, lower], axis=0)


def dot(left, right):
    return jnp.dot(left, right, preferred_element_type=jnp.float32)


def split(block):
    high = block.astype(jnp.bfloat16)
    low = (block - high.astype(jnp.float32)).astype(jnp.bfloat16)
    return high, low


def fine_dot(left, right):
    return dot(left[0], right[0]) + (dot(left[0], right[1]) + dot(left[1], right[0]))


def product(left, right):
    return fine_dot(split(embed(left)), split(right))


def unit(size):
    rows = lax.broadcasted_iota(jnp.int32, (2 * size, size), 0)
    cols = lax.broadcasted_iota(jnp.int32, (2 * size, size), 1)
    return jnp.where(rows == cols, 1.0, 0.0).astype(jnp.float32)


def total(block):
    return jnp.sum(jnp.sum(block, axis=0, keepdims=True), axis=1, keepdims=True)[0, 0]


def peak(block):
    return jnp.max(jnp.max(block, axis=0, keepdims=True), axis=1, keepdims=True)[0, 0]


def invert(systems, scratch):
    size = systems[0].shape[1]
    one = unit(size)
    narrow = jnp.bfloat16
    count = len(systems)
    exact = []
    worst = None
    for k, p in enumerate(systems):
        x_ref, r_ref = scratch[k]
        first = one + p
        p_embed = embed(halves(p)).astype(narrow)
        square = dot(p_embed, p.astype(narrow))
        square_embed = embed(halves(square)).astype(narrow)
        second = first + dot(embed(halves(first)).astype(narrow), square.astype(narrow))
        fourth = dot(square_embed, square.astype(narrow))
        x = second + dot(embed(halves(second)).astype(narrow), fourth.astype(narrow))
        a = one - p
        a_split = split(embed(halves(a)))
        r = one - fine_dot(a_split, split(x))
        x_ref[...] = x
        r_ref[...] = r
        norm = total(r * r)
        worst = norm if worst is None else jnp.maximum(worst, norm)
        exact.append((a, a_split))

    def restart():
        norm = jnp.float32(0.0)
        for k in range(count):
            a, a_split = exact[k]
            x_ref, r_ref = scratch[k]
            full = jnp.abs(embed(halves(a)))
            scale = peak(jnp.sum(full, axis=0, keepdims=True)) * peak(
                jnp.sum(full, axis=1, keepdims=True)
            )
            real, imaginary = halves(a)
            x = jnp.concatenate([real.T, -imaginary.T], axis=0) / scale
            r = one - fine_dot(a_split, split(x))
            x_ref[...] = x
            r_ref[...] = r
            norm = jnp.maximum(norm, total(r * r))
        return norm

    worst = lax.cond(worst < 0.25, lambda: worst, restart)

    def unfinished(state):
        return jnp.logical_and(state[0] > 3e-3, state[1] < 200)

    def improve(state):
        norm = jnp.float32(0.0)
        for k in range(count):
            x_ref, r_ref = scratch[k]
            x = x_ref[...]
            x = x + product(halves(x), r_ref[...])
            r = one - fine_dot(exact[k][1], split(x))
            x_ref[...] = x
            r_ref[...] = r
            norm = jnp.maximum(norm, total(r * r))
        return norm, state[1] + 1

    lax.while_loop(unfinished, improve, (worst, jnp.int32(0)))
    inverses = []
    for x_ref, r_ref in scratch[:count]:
        x, r = x_ref[...], r_ref[...]
        square = dot(embed(halves(r)).astype(narrow), r.astype(narrow))
        x = x + product(halves(x), r)
        inverses.append(x + dot(embed(halves(x)).astype(narrow), square.astype(narrow)))
    return inverses


def prepare(former, latter, tables):
    outer_a, inner_a, outer_b, inner_b = tables
    size = len(inner_a)
    from_former = take(former, inner_a, np.concatenate([inner_a, outer_a]))
    reflected = product(take(latter, inner_b, inner_b), stack(from_former))
    right_side = jnp.concatenate(
        [reflected[:, size:], -stack(take(latter, inner_b, outer_b))], axis=1
    )
    return reflected[:, :size], right_side


def finish(former, latter, tables, inverse, right_side):
    outer_a, inner_a, outer_b, inner_b = tables
    size_former, size_latter = len(outer_a), len(outer_b)
    solved = product(halves(inverse), right_side)
    rows = np.concatenate([outer_a, inner_a])
    passed = product(take(former, rows, inner_a), solved)
    upper, traces = [], []
    for part, own in zip(halves(passed), take(former, rows, outer_a)):
        wide = jnp.concatenate([own, jnp.zeros((len(rows), size_latter), jnp.float32)], axis=1)
        part = part + wide
        upper.append(part[:size_former])
        traces.append(part[size_former:])
    coupled = product(take(latter, outer_b, inner_b), stack(traces))
    merged = []
    for high, part, own in zip(upper, halves(coupled), take(latter, outer_b, outer_b)):
        wide = jnp.concatenate([jnp.zeros((size_latter, size_former), jnp.float32), own], axis=1)
        merged.append(jnp.concatenate([high, wide - part], axis=0))
    return tuple(merged)


def merge_pair(former, latter, tables, scratch):
    system, right_side = prepare(former, latter, tables)
    (inverse,) = invert([system], [scratch])
    return finish(former, latter, tables, inverse, right_side)


def sides(own_ref, partner_ref, swapped):
    former, latter = [], []
    for part in range(2):
        own, other = own_ref[part], partner_ref[part]
        former.append(jnp.where(swapped, other, own))
        latter.append(jnp.where(swapped, own, other))
    return tuple(former), tuple(latter)


def box_kernel(fine_set, flag_ref, coarse_ref, fine_ref, out_ref, *scratch):
    left_tab, right_tab, whole_tab, order = fine_set
    pairs = [scratch[0:2], scratch[2:4], scratch[4:6]]

    @pl.when(flag_ref[0, 0] > 0)
    def _():
        pieces = [(fine_ref[k, 0], fine_ref[k, 1]) for k in range(4)]
        left_system, left_side = prepare(pieces[0], pieces[1], left_tab)
        right_system, right_side = prepare(pieces[2], pieces[3], right_tab)
        left_inverse, right_inverse = invert([left_system, right_system], pairs)
        left_map = finish(pieces[0], pieces[1], left_tab, left_inverse, left_side)
        right_map = finish(pieces[2], pieces[3], right_tab, right_inverse, right_side)
        whole = take(merge_pair(left_map, right_map, whole_tab, pairs[2]), order, order)
        out_ref[0] = whole[0]
        out_ref[1] = whole[1]

    @pl.when(flag_ref[0, 0] <= 0)
    def _():
        out_ref[...] = coarse_ref[...]


def pair_kernel(tables, place_ref, own_ref, partner_ref, out_ref, *scratch):
    former, latter = sides(own_ref, partner_ref, place_ref[0] > 0)
    merged = merge_pair(former, latter, tables, scratch)
    out_ref[0] = merged[0]
    out_ref[1] = merged[1]


def half_kernel(tables, next_tables, place_ref, own_ref, partner_ref, face_ref, outward_ref, rows_ref, *scratch):
    former, latter = sides(own_ref, partner_ref, place_ref[0] > 0)
    merged = merge_pair(former, latter, tables, scratch)
    outer_a, inner_a, outer_b, inner_b = next_tables
    latter_side = place_ref[1] > 0
    second_rows = place_ref[2] > 0
    second_cols = place_ref[3] > 0
    size = len(inner_a)
    tile = rows_ref.shape[1]
    near = np.concatenate([inner_a, outer_a])
    far = np.concatenate([inner_b, outer_b])
    for part in range(2):
        chosen = jnp.where(
            latter_side,
            pick(pick(merged[part], far, 0), far, 1),
            pick(pick(merged[part], near, 0), near, 1),
        )
        low, high = size + tile, size + 2 * tile
        cols = jnp.where(second_cols, chosen[:, low:high], chosen[:, size:low])
        face_ref[part] = chosen[:size, :size]
        outward_ref[part] = cols[:size]
        coupling = chosen[:, :size]
        rows_ref[part, :, :size] = jnp.where(second_rows, coupling[low:high], coupling[size:low])
        rows_ref[part, :, size:] = jnp.where(second_rows, cols[low:high], cols[size:low])


def tile_kernel(place_ref, face_ref, outward_ref, got_face_ref, got_outward_ref, rows_ref, out_ref, *scratch):
    latter_side = place_ref[1] > 0
    latter_tile = place_ref[4] > 0
    size = face_ref.shape[1]
    former = [jnp.where(latter_side, got_face_ref[k], face_ref[k]) for k in range(2)]
    latter = [jnp.where(latter_side, face_ref[k], got_face_ref[k]) for k in range(2)]
    same = latter_side == latter_tile
    outward = stack([jnp.where(same, outward_ref[k], got_outward_ref[k]) for k in range(2)])
    reflected = product(latter, jnp.concatenate([stack(former), outward], axis=1))
    (inverse,) = invert([reflected[:, :size]], [scratch])
    right_side = jnp.where(latter_tile, -outward, reflected[:, size:])
    solved = product(halves(inverse), right_side)
    traces = product(former, solved) + jnp.where(latter_tile, 0.0, outward)
    applied = jnp.where(latter_side, -traces, solved)
    coupling = [rows_ref[k, :, :size] for k in range(2)]
    through = halves(product(coupling, applied))
    for k in range(2):
        out_ref[k] = through[k] + jnp.where(same, rows_ref[k, :, size:], 0.0)


def flipped(index, bit):
    step = 2**bit
    return index + step * (1 - 2 * lax.rem(lax.div(index, step), 2))


def hop(source, target, sems, slot, device):
    return pltpu.make_async_remote_copy(
        src_ref=source,
        dst_ref=target,
        send_sem=sems[0].at[slot],
        recv_sem=sems[1].at[slot],
        device_id=device,
        device_id_type=pl.DeviceIdType.MESH,
    )


def greet(devices):
    barrier = pltpu.get_barrier_semaphore()
    for device in devices:
        pl.semaphore_signal(
            barrier, inc=1, device_id=device, device_id_type=pl.DeviceIdType.MESH
        )
    pl.semaphore_wait(barrier, len(devices))


def swap_kernel(axis, bit, chunks, own_ref, out_ref, far_send, far_recv, near_send, near_recv):
    gx, gy = lax.axis_index("gx"), lax.axis_index("gy")
    peer = (flipped(gx, bit), gy) if axis == "gx" else (gx, flipped(gy, bit))
    sibling = (gx, flipped(gy, 0))
    mine = lax.rem(gy, 2)
    greet([peer, sibling])
    rows = own_ref.shape[1] // chunks
    far, near = (far_send, far_recv), (near_send, near_recv)
    out, relays = [], []
    for k in range(chunks):
        spot = (mine, pl.ds(k * rows, rows))
        copy = hop(own_ref.at[spot], out_ref.at[spot], far, k, peer)
        copy.start()
        out.append(copy)
        relays.append(hop(out_ref.at[spot], out_ref.at[spot], near, k, sibling))
    for k in range(chunks):
        out[k].wait_recv()
        relays[k].start()
    for k in range(chunks):
        relays[k].wait_recv()
    for k in range(chunks):
        out[k].wait_send()
        relays[k].wait_send()


def line_kernel(face_ref, outward_ref, got_face_ref, got_outward_ref, far_send, far_recv, on_send, on_recv, near_send, near_recv):
    gx, gy = lax.axis_index("gx"), lax.axis_index("gy")
    low, second = lax.rem(gx, 2), lax.rem(lax.div(gx, 2), 2)
    middle = low != second
    across = (gx + 1 - 2 * second, gy)
    along = (flipped(gx, 0), gy)
    sibling = (gx, flipped(gy, 0))
    mine = lax.rem(gy, 2)
    group = lax.rem(lax.div(gy, 2), 2)
    gives = group == second
    takes = group != second

    @pl.when(middle)
    def _():
        greet([across, along, sibling])

    @pl.when(jnp.logical_not(middle))
    def _():
        greet([along, sibling])

    rows = outward_ref.shape[1] // 2
    spots = [(part, pl.ds(k * rows, rows)) for part in range(2) for k in range(2)]
    far, on, near = (far_send, far_recv), (on_send, on_recv), (near_send, near_recv)
    face_far = hop(face_ref.at[mine], got_face_ref.at[mine], far, 0, across)
    face_on = hop(got_face_ref.at[mine], got_face_ref.at[mine], on, 0, along)
    face_near = hop(got_face_ref.at[mine], got_face_ref.at[mine], near, 0, sibling)
    cols_far = [
        hop(outward_ref.at[spot], got_outward_ref.at[spot], far, k + 1, across)
        for k, spot in enumerate(spots)
    ]
    cols_on = [
        hop(got_outward_ref.at[spot], got_outward_ref.at[spot], on, k + 1, along)
        for k, spot in enumerate(spots)
    ]

    @pl.when(middle)
    def _():
        face_far.start()

        @pl.when(gives)
        def _():
            for copy in cols_far:
                copy.start()

        face_far.wait_recv()
        face_on.start()
        face_near.start()

        @pl.when(takes)
        def _():
            for first, then in zip(cols_far, cols_on):
                first.wait_recv()
                then.start()
            for then in cols_on:
                then.wait_send()

        @pl.when(gives)
        def _():
            for copy in cols_far:
                copy.wait_send()

        face_far.wait_send()
        face_on.wait_send()

    @pl.when(jnp.logical_not(middle))
    def _():
        face_on.wait_recv()
        face_near.start()

        @pl.when(takes)
        def _():
            for copy in cols_on:
                copy.wait_recv()

    face_near.wait_recv()
    face_near.wait_send()


def exchange(kernel, identity, copies, *blocks):
    vmem = pl.BlockSpec(memory_space=pltpu.VMEM)
    outs = [jax.ShapeDtypeStruct(block.shape, block.dtype) for block in blocks]
    single = len(outs) == 1
    return pl.pallas_call(
        kernel,
        out_shape=outs[0] if single else tuple(outs),
        in_specs=[vmem] * len(blocks),
        out_specs=vmem if single else tuple([vmem] * len(outs)),
        scratch_shapes=[pltpu.SemaphoreType.DMA((count,)) for count in copies for _ in range(2)],
        compiler_params=pltpu.CompilerParams(collective_id=identity, has_side_effects=True, vmem_limit_bytes=4 * 1024 * 1024),
    )(*blocks)


def swap(block, axis, bit, identity):
    chunks = 4
    return exchange(
        functools.partial(swap_kernel, axis, bit, chunks), identity, (chunks, chunks), block
    )


def work(*sizes):
    return [pltpu.VMEM((2 * size, size), jnp.float32) for size in sizes for _ in range(2)]


def call(kernel, shapes, scratch, place, *blocks):
    vmem = pl.BlockSpec(memory_space=pltpu.VMEM)
    outs = [jax.ShapeDtypeStruct(shape, jnp.float32) for shape in shapes]
    single = len(outs) == 1
    return pl.pallas_call(
        kernel,
        out_shape=outs[0] if single else tuple(outs),
        in_specs=[pl.BlockSpec(memory_space=pltpu.SMEM)] + [vmem] * len(blocks),
        out_specs=vmem if single else tuple([vmem] * len(outs)),
        scratch_shapes=scratch,
        compiler_params=pltpu.CompilerParams(vmem_limit_bytes=12 * 1024 * 1024),
    )(place, *blocks)


def body(coarse_map, fine_maps, pml_flag):
    points = coarse_map.shape[-1] // 4
    fine_set = fine_tables(points)
    sections = level_tables(points)
    inner = [len(section[1]) for section in sections]
    width = [len(section[0]) + len(section[2]) for section in sections]
    tile = 4 * points
    gx_index = lax.axis_index("gx")
    gy_index = lax.axis_index("gy")

    def place(swapped):
        return jnp.stack(
            [
                swapped,
                gx_index // 2 % 2,
                gx_index % 2,
                gy_index % 2,
                gy_index // 2 % 2,
            ]
        ).astype(jnp.int32)

    boxed = call(
        functools.partial(box_kernel, fine_set),
        [coarse_map.shape[2:]],
        work(points // 2, points // 2, points),
        pml_flag,
        coarse_map[0, 0],
        fine_maps[0, 0],
    )
    one = call(
        functools.partial(pair_kernel, sections[0]),
        [(2, width[0], width[0])],
        work(inner[0]),
        place(gy_index % 2),
        boxed,
        partner(boxed, "gy", 0),
    )
    two = call(
        functools.partial(pair_kernel, sections[1]),
        [(2, width[1], width[1])],
        work(inner[1]),
        place(gx_index % 2),
        one,
        swap(one, "gx", 0, 0),
    )
    face, outward, own_rows = call(
        functools.partial(half_kernel, sections[2], sections[3]),
        [(2, inner[3], inner[3]), (2, inner[3], tile), (2, tile, inner[3] + tile)],
        work(inner[2]),
        place(gy_index // 2 % 2),
        two,
        swap(two, "gy", 1, 1),
    )
    got_face, got_outward = exchange(line_kernel, 2, (5, 5, 1), face, outward)
    return call(
        tile_kernel,
        [(2, tile, tile)],
        work(inner[3]),
        place(gx_index // 2 % 2),
        face,
        outward,
        got_face,
        got_outward,
        own_rows,
    )


def solution(mesh):
    placed = (P("gx", "gy", None, None, None), P("gx", "gy", None, None, None, None), P("gx", "gy"))
    return jax.shard_map(
        body, mesh=mesh, in_specs=placed, out_specs=P(None, "gx", "gy"), check_vma=False
    )
```
